32 devices in a mesh: row: 8 (over z, y), col: 4 (over x, core).
Axes of the slice: x: 2, y: 2, z: 4, core: 2. Of those that a mesh axis runs over, the one named last changes fastest.
Arguments:
- tokens: bfloat16 [256, 7168], P(('row', 'col')), may hold values from -6 to 6
- gate_weights: bfloat16 [256, 4], P(('row', 'col')), may hold values from 0.099609375 to 1
- expert_ids: int32 [256, 4], P(('row', 'col')), may hold values from 0 to 7, all different within a row; in each aligned block of 32 rows (0 to 31, 32 to 63, ...) at most 24 rows name the same one
- w_in: bfloat16 [4, 7168, 2, 4096], P('col', None, None, 'row'), may hold values from -0.0625 to 0.0625
- w_out: bfloat16 [4, 4096, 7168], P('col', 'row'), may hold values from -0.125 to 0.125
Outputs:
- combined: bfloat16 [256, 7168], P(('row', 'col'))
The draws below stay inside these ranges and needn't reach their ends.
Inputs may be any that keep to these rules, and one draw needn't show every extreme that they name: `expert_ids`: each token names 4 different experts; in every aligned block of 32 rows (one token group) no expert is named by more than 24 rows, a bound that some block reaches.
All inputs are finite; a program needn't handle non-finite values.
Results may differ from the reference program's by a relative error of at most 0.018.
Values may be sent and summed in bfloat16 or wider, within the bound.
No kernel may reach another device: no remote copies, remote signals or barrier semaphores. Data moves between devices by JAX's collectives and lax.ppermute only.
A program may use at most 128 MiB of HBM per device.

```python
import math
import jax
import jax.numpy as jnp
import numpy as np
from jax import lax

D = 7168
FF = 2048
TOP = 4
EXP_DEV = 2
CAP = 24
EXPERTS = 8
BLOCK = 32
TOKENS = 256
N_ROW = 8


def block_scale(rng, shape, pieces, smallest, top_value):
    gain, own = 1.0, jax.random.fold_in(rng, 6)
    for dim, shards_of in pieces:
        steps = jnp.exp(jax.random.uniform(jax.random.fold_in(own, dim), (shards_of,), jnp.float32, smallest / len(pieces), top_value / len(pieces)))
        gain = gain * jnp.repeat(steps, shape[dim] // shards_of).reshape([-1 if axis == dim else 1 for axis in range(len(shape))])
    return gain


def shared_out(key, own, number, rows, amount, top, limit, lean):
    sequence = jax.random.permutation(key, amount)
    heavy_load, usual = load_shares(amount, rows * top, limit, lean, True), load_shares(amount, rows * top, limit, lean, False)
    places = jnp.arange(amount)

    def named(sizes, offset_by):
        used = int((sizes > 0).sum())
        fixed = max(1, used // 4)
        moved = fixed + (places - fixed + offset_by * (used - fixed)) % max(1, amount - fixed)
        return jnp.zeros((amount,), jnp.int32).at[sequence[jnp.where(places < fixed, places, moved)]].set(jnp.asarray(sizes, jnp.int32))

    sizes = jnp.where(number % 4 == 0, named(heavy_load, number // 4), named(usual, number - number // 4 - 1))
    mixed = jax.random.permutation(jax.random.fold_in(own, 3), amount)
    giver, taker = mixed[0:amount // 2 * 2:2], mixed[1:amount // 2 * 2:2]
    slack = jnp.minimum(sizes[giver] - 1, limit - sizes[taker]) // 2
    slack = jnp.where((giver == sequence[0]) | (taker == sequence[0]) | (sizes[taker] == 0), 0, jnp.maximum(slack, 0))
    moved = jax.random.randint(jax.random.fold_in(own, 4), (amount // 2,), 0, 1 << 20) % (slack + 1)
    sizes = sizes.at[giver].add(-moved).at[taker].add(moved)
    labels = jnp.searchsorted(jnp.cumsum(sizes), jnp.arange(rows * top), side="right").astype(jnp.int32)
    table = labels.reshape(top, rows).T
    table = table[jax.random.permutation(jax.random.fold_in(own, 1), rows)]
    offset_by = jax.random.randint(jax.random.fold_in(own, 2), (rows, 1), 0, top)
    return jnp.take_along_axis(table, (jnp.arange(top)[None, :] + offset_by) % top, axis=1)


def load_shares(number_of, total, reach, lean, full):
    weights = [(1 << 20) // math.isqrt(rank ** lean) + 1 for rank in range(1, number_of + 1)]
    largest = reach if full else min(reach, max(-(-total // number_of), total * weights[0] // sum(weights)))
    least = 1 if total - largest >= number_of - 1 else 0
    counts, spare = [largest] + [least] * (number_of - 1), total - largest - least * (number_of - 1)
    while spare > 0:
        free = [i for i in range(1, number_of) if counts[i] < largest] or [i for i in range(1, number_of) if counts[i] < reach]
        mass, budget = sum([weights[i] for i in free]), spare
        for i in free:
            addition = min(reach - counts[i], max(1, budget * weights[i] // mass), spare)
            counts[i] = counts[i] + addition
            spare = spare - addition
    return np.array(counts)


def noise(rng, dims, spread, most, pieces=(), kind=jnp.bfloat16):
    level = block_scale(rng, dims, pieces, -0.22, 0.18) if pieces else 1.0
    values = jax.random.normal(rng, dims, jnp.float32) * spread * level
    return jnp.minimum(jnp.maximum(values, -most), most).astype(kind)


def setup_inputs(seed: int = 0) -> dict:
    arg_keys = jax.random.split(jax.random.key(seed), 6)
    tokens = noise(arg_keys[0], (TOKENS, D), 1.0, 6.0, ((0, 32),))
    gate_weights = jnp.clip(0.099609375 + 0.9003906 * jax.random.uniform(arg_keys[1], (TOKENS, TOP), jnp.float32) ** block_scale(arg_keys[1], (TOKENS, TOP), ((0, 32),), -0.2, 0.2), 0.099609375, 1.0).astype(jnp.bfloat16)
    expert_ids_keys = jax.random.split(jax.random.fold_in(arg_keys[2], 1), TOKENS // BLOCK)
    expert_ids_turns = jax.random.permutation(jax.random.fold_in(arg_keys[2], 3), TOKENS // BLOCK)
    expert_ids = jax.vmap(lambda own, number: shared_out(jax.random.fold_in(arg_keys[2], 2), own, number, BLOCK, EXPERTS, TOP, CAP, 2))(expert_ids_keys, expert_ids_turns).reshape((TOKENS, TOP))
    w_in = noise(arg_keys[3], (EXPERTS // EXP_DEV, D, 2, EXP_DEV * FF), D ** -0.5, 0.0625, ((0, 4), (3, 8)))
    w_out = noise(arg_keys[4], (EXPERTS // EXP_DEV, EXP_DEV * FF, D), FF ** -0.5, 0.125, ((0, 4), (1, 8)))
    return {"tokens": tokens, "gate_weights": gate_weights, "expert_ids": expert_ids, "w_in": w_in, "w_out": w_out}


def reference(tokens, gate_weights, expert_ids, w_in, w_out):
    block_count = TOKENS // BLOCK
    route_ids = expert_ids.reshape(block_count, BLOCK, TOP)
    experts = jnp.arange(EXPERTS, dtype=jnp.int32)
    member = jnp.any(route_ids[:, :, :, None] == experts[None, None, None, :], axis=2).astype(jnp.int32)
    slot_index = jnp.cumsum(member, axis=1) - member
    slot_target = jnp.where(member > 0, slot_index, CAP).astype(jnp.int32)
    block_grid = jnp.broadcast_to(jnp.arange(block_count, dtype=jnp.int32)[:, None, None], member.shape)
    expert_grid = jnp.broadcast_to(experts[None, None, :], member.shape)
    token_grid = jnp.broadcast_to(jnp.arange(BLOCK, dtype=jnp.int32)[None, :, None], member.shape)
    slot_table = jnp.full((EXPERTS, block_count, CAP), BLOCK, jnp.int32)
    slot_table = slot_table.at[expert_grid, block_grid, slot_target].set(token_grid, mode="drop")
    padded_tokens = jnp.concatenate([tokens.reshape(block_count, BLOCK, D), jnp.zeros((block_count, 1, D), tokens.dtype)], axis=1)
    piece_count = N_ROW // EXP_DEV
    unit_width = EXP_DEV * FF // N_ROW
    block_range = jnp.arange(block_count, dtype=jnp.int32)

    def one_expert(expert):
        column = (expert // EXP_DEV).astype(jnp.int32)
        within = (expert % EXP_DEV).astype(jnp.int32)
        token_rows = padded_tokens[block_range[:, None], slot_table[expert]].reshape(block_count * CAP, D)
        in_weights = lax.dynamic_slice_in_dim(w_in[column], within * FF, FF, 2)
        gate_up = jnp.dot(token_rows, in_weights.reshape(D, 2 * FF), preferred_element_type=jnp.float32)
        gate_up = gate_up.reshape(block_count * CAP, 2, FF)
        hidden = (jax.nn.silu(gate_up[:, 0]) * gate_up[:, 1]).astype(jnp.bfloat16)
        out_weights = lax.dynamic_slice_in_dim(w_out[column], within * FF, FF, 0)
        running = jnp.zeros((block_count * CAP, D), jnp.float32)
        for segment in range(piece_count):
            partial_value = jnp.dot(hidden[:, segment * unit_width:(segment + 1) * unit_width], out_weights[segment * unit_width:(segment + 1) * unit_width], preferred_element_type=jnp.float32)
            running = running + lax.optimization_barrier(partial_value.astype(jnp.bfloat16)).astype(jnp.float32)
        return running.astype(jnp.bfloat16).reshape(block_count, CAP, D)

    outputs = lax.map(one_expert, experts)
    pair_slot = jnp.take_along_axis(slot_index, route_ids, axis=2)
    gate_values = gate_weights.reshape(block_count, BLOCK, TOP).astype(jnp.float32)
    combined = jnp.zeros((block_count, BLOCK, D), jnp.float32)
    for choice_k in range(TOP):
        picked = outputs[route_ids[:, :, choice_k], block_range[:, None], pair_slot[:, :, choice_k]]
        combined = combined + gate_values[:, :, choice_k, None] * picked.astype(jnp.float32)
    return combined.reshape(TOKENS, D).astype(jnp.bfloat16)
```

```python
import jax
import jax.numpy as jnp
from jax import lax
from jax.sharding import PartitionSpec as P

EXP_DEV = 2
LANES = 128
AXES = ("row", "col")


def solution(mesh):
    rows, cols = mesh.shape["row"], mesh.shape["col"]
    sizes = {"z": rows // 2, "y": 2, "x": cols // 2, "c": 2}
    names = tuple(sizes)
    strides = {"c": 1, "x": 2, "y": cols, "z": 2 * cols}
    devices = rows * cols

    def swap(value, axis, distance):
        pairs = []
        for here in range(devices):
            place = here // strides[axis] % sizes[axis]
            pairs.append((here, here + ((place ^ distance) - place) * strides[axis]))
        return lax.ppermute(value, AXES, pairs)

    def gather(block, axis, at):
        got = {r: swap(block, axis, r) for r in reversed(range(1, sizes[axis]))}
        return jnp.stack([block] + [got[r] for r in range(1, sizes[axis])], axis=at)

    def scatter(value, axis, at):
        entry = lambda r: lax.index_in_dim(value, r, at, keepdims=False)
        got = [swap(entry(r), axis, r) for r in reversed(range(1, sizes[axis]))]
        total = entry(0).astype(jnp.float32)
        for part in got:
            total = total + part.astype(jnp.float32)
        return total.astype(jnp.bfloat16)

    def on_device(tokens, gate_weights, expert_ids, w_in, w_out):
        count, width = tokens.shape
        units = w_out.shape[1]
        experts = jnp.arange(LANES, dtype=jnp.int32)
        chosen = expert_ids[:, None, :] == experts[None, :, None]
        table = jnp.sum(jnp.where(chosen, gate_weights[:, None, :], 0), axis=2)
        packed = jnp.concatenate([tokens, table.astype(jnp.bfloat16)], axis=1)
        half = width // (2 * LANES) * LANES

        held = gather(packed, "z", 0)
        first, second = held[..., :half], held[..., half:]
        first = gather(gather(first, "x", 0), "y", 1)
        second = gather(gather(second, "y", 0), "x", 0)
        first = gather(first, "c", 0).reshape(-1, half)
        second = gather(second, "c", 0).reshape(-1, width + LANES - half)
        total = devices * count

        mine = lax.axis_index("col") * EXP_DEV + lax.axis_index("row") // (rows // EXP_DEV)
        gates = lax.dynamic_slice_in_dim(second, width - half + mine, 1, 1).astype(jnp.float32)
        everything = jnp.concatenate([first, second[:, : width - half]], axis=1)
        gate_up = jnp.dot(
            everything, w_in[0].reshape(width, 2 * units), preferred_element_type=jnp.float32
        )
        hidden = jax.nn.silu(gate_up[:, :units]) * gate_up[:, units:]
        hidden = hidden.astype(jnp.bfloat16)
        partial = jnp.dot(hidden, w_out[0], preferred_element_type=jnp.float32)
        partial = (partial * gates).astype(jnp.bfloat16)

        partial = partial.reshape(2, sizes["x"], 2, sizes["z"], count, width)
        partial = scatter(partial, "c", 0)
        first, second = partial[..., :half], partial[..., half:]
        first = scatter(scatter(first, "x", 0), "y", 0)
        second = scatter(scatter(second, "y", 1), "x", 0)
        return jnp.concatenate([scatter(first, "z", 0), scatter(second, "z", 0)], axis=1)

    return jax.shard_map(
        on_device,
        mesh=mesh,
        in_specs=(
            P(AXES, None),
            P(AXES, None),
            P(AXES, None),
            P("col", None, None, "row"),
            P("col", "row", None),
        ),
        out_specs=P(AXES, None),
        check_vma=False,
    )
```

```python
import functools

import jax
import jax.numpy as jnp
from jax import lax
from jax.experimental import pallas as pl
from jax.experimental.pallas import tpu as pltpu
from jax.sharding import PartitionSpec as P

EXP_DEV = 2
LANES = 128
AXES = ("row", "col")
RING = 4
IN_VMEM = pl.BlockSpec(memory_space=pltpu.VMEM)
IN_HBM = pl.BlockSpec(memory_space=pltpu.HBM)
IN_SMEM = pl.BlockSpec(memory_space=pltpu.SMEM)


def gate_up_kernel(pieces, step, units, first_step, last, *refs):
    token_refs, weights = refs[:pieces], refs[pieces]
    if last:
        before, mine, out = refs[pieces + 1 : pieces + 4]
    else:
        out = refs[pieces + 1]
    landing, arrived, even, odd, total = refs[-5:]
    per = 2 * units // LANES
    block = per * step
    steps = (token_refs[0].shape[1] - (LANES if last else 0)) // step
    wide = (even, odd)

    def fetch(k):
        return pltpu.make_async_copy(
            weights.at[pl.ds((first_step + k) * block, block), :],
            landing.at[k % RING],
            arrived.at[k % RING],
        )

    def unpack(k):
        fetch(k).wait()
        piece = min(block, 512)
        for at in range(0, block, piece):
            wide[k % 2][pl.ds(at, piece), :] = landing[k % RING, pl.ds(at, piece), :].astype(
                jnp.float32
            )
        if k + RING < steps:
            fetch(k + RING).start()

    for k in range(min(RING, steps)):
        fetch(k).start()
    total[...] = before[...] if last else jnp.zeros_like(total)
    unpack(0)
    for k in range(steps):
        if k + 1 < steps:
            unpack(k + 1)
        tokens = jnp.concatenate([ref[:, k * step : (k + 1) * step] for ref in token_refs], axis=0)
        for g in range(2):
            columns = [
                wide[k % 2][pl.ds(2 * f + g, step, stride=per), :].astype(jnp.bfloat16)
                for f in range(units // LANES)
            ]
            total[:, g * units : (g + 1) * units] += jnp.dot(
                tokens, jnp.concatenate(columns, axis=1), preferred_element_type=jnp.float32
            )
    if not last:
        out[...] = total[...]
        return
    table = jnp.concatenate([ref[:, -LANES:] for ref in token_refs], axis=0).astype(jnp.float32)
    lane = lax.broadcasted_iota(jnp.int32, table.shape, 1)
    gates = jnp.sum(jnp.where(lane == mine[0], table, 0.0), axis=1, keepdims=True)
    gate = total[:, :units]
    out[...] = (gate / (1 + jnp.exp(-gate)) * total[:, units:] * gates).astype(jnp.bfloat16)


def gate_up(pieces, weights, units, step, start, before=None, mine=None):
    last = before is not None
    rows = sum(piece.shape[0] for piece in pieces)
    depth = pieces[0].shape[1] - (LANES if last else 0)
    block = 2 * units // LANES * step
    shape = (rows, units if last else 2 * units)
    return pl.pallas_call(
        functools.partial(gate_up_kernel, len(pieces), step, units, start // step, last),
        out_shape=jax.ShapeDtypeStruct(shape, jnp.bfloat16 if last else jnp.float32),
        in_specs=[IN_VMEM] * len(pieces) + [IN_HBM] + ([IN_VMEM, IN_SMEM] if last else []),
        out_specs=IN_VMEM,
        scratch_shapes=[
            pltpu.VMEM((RING, block, LANES), jnp.bfloat16),
            pltpu.SemaphoreType.DMA((RING,)),
            pltpu.VMEM((block, LANES), jnp.float32),
            pltpu.VMEM((block, LANES), jnp.float32),
            pltpu.VMEM((rows, 2 * units), jnp.float32),
        ],
        compiler_params=pltpu.CompilerParams(vmem_limit_bytes=min(60 << 20, (16 << 20) + (rows * 24 << 10))),
        cost_estimate=pl.CostEstimate(
            flops=4 * rows * depth * units, bytes_accessed=4 * depth * units, transcendentals=0
        ),
        name="gate_up_last" if last else "gate_up",
    )(*pieces, weights, *((before, mine) if last else ()))


def solution(mesh):
    rows, cols = mesh.shape["row"], mesh.shape["col"]
    devices = rows * cols
    core, x, y = 1, 2, cols
    upper = [cols * 2 * r for r in range(rows // 2)]
    beside = [4 * r for r in range(cols // 4)]

    def swap(value, flip):
        return lax.ppermute(value, AXES, [(here, here ^ flip(here)) for here in range(devices)])

    def near(stage):
        return lambda here: (x, y)[(stage + here) % 2]

    def far(flips):
        return sorted((f for f in flips if f), reverse=True)

    def gather(held, flips):
        got = {f: swap(held, lambda here, f=f: f) for f in far(flips)}
        return jnp.concatenate([held] + [got[f] for f in flips if f], axis=0)

    def add(first, *rest):
        total = first.astype(jnp.float32)
        for part in rest:
            total = total + part.astype(jnp.float32)
        return total.astype(jnp.bfloat16)

    def scatter(sums, flips):
        size = sums.shape[0] // len(flips)
        part = {f: sums[r * size : (r + 1) * size] for r, f in enumerate(flips)}
        got = [swap(part[f], lambda here, f=f: f) for f in far(flips)]
        return add(part[0], *got)

    def collect(own):
        held = gather(gather(own, upper), beside)
        held = jnp.concatenate([held, swap(held, near(0))], axis=0)
        received = swap(held, near(1))
        other = lambda here: core
        return [held, received, swap(held, other), swap(received, other)]

    def combine(sums):
        mine, others = sums
        mine = add(mine, swap(others, lambda here: core))
        size = mine.shape[0] // 2
        mine = add(mine[:size], swap(mine[size:], near(1)))
        size = size // 2
        mine = add(mine[:size], swap(mine[size:], near(0)))
        return scatter(scatter(mine, beside), upper)

    def on_device(tokens, gate_weights, expert_ids, w_in, w_out):
        width = tokens.shape[1]
        units = w_out.shape[1]
        half = width // 2 // LANES * LANES
        step = next(s for s in (512, 256, LANES) if half % s == 0 and (width - half) % s == 0)
        chosen = expert_ids[:, None, :] == jnp.arange(LANES, dtype=jnp.int32)[None, :, None]
        table = jnp.sum(jnp.where(chosen, gate_weights[:, None, :], 0), axis=2).astype(jnp.bfloat16)
        first = collect(tokens[:, :half])
        second = collect(jnp.concatenate([tokens[:, half:], table], axis=1))

        lanes = units // LANES
        weights = w_in[0].reshape(width, 2, lanes, LANES).transpose(0, 2, 1, 3)
        weights = weights.reshape(width * 2 * lanes, LANES)
        mine = lax.axis_index("col") * EXP_DEV + lax.axis_index("row") // (rows // EXP_DEV)
        total = gate_up(first, weights, units, step, 0)
        hidden = gate_up(second, weights, units, step, half, total, mine.reshape(1))
        size = hidden.shape[0] // 2
        outs = []
        for at, to in ((0, half), (half, width)):
            part = jnp.dot(hidden, w_out[0][:, at:to], preferred_element_type=jnp.float32)
            part = part.astype(jnp.bfloat16)
            outs.append(combine((part[:size], part[size:])))
        return jnp.concatenate(outs, axis=1)

    return jax.shard_map(
        on_device,
        mesh=mesh,
        in_specs=(
            P(AXES, None),
            P(AXES, None),
            P(AXES, None),
            P("col", None, None, "row"),
            P("col", "row", None),
        ),
        out_specs=P(AXES, None),
        check_vma=False,
    )
```
